256 devices in a mesh: bev: 64 (over z, x, core), scene: 4 (over y).
Axes of the slice: x: 4, y: 4, z: 8, core: 2. Of those that a mesh axis runs over, the one named last changes fastest.
Arguments:
- context: bfloat16 [4, 80, 16384], P('scene', None, 'bev'), may hold values from -24 to 24
- depth_logits: float32 [4, 112, 16384], P('scene', None, 'bev'), may hold values from -20 to 300
- send_count: int32 [4, 64, 64], P('scene', 'bev'), may hold values from 0 to 1024, as said below
- slot_point: int32 [4, 64, 64, 1024], P('scene', 'bev'), may hold values from 0 to 28671, as said below
- slot_cell: int32 [4, 64, 64, 1024], P('scene', 'bev'), may hold values from 0 to 255
Outputs:
- bev_features: bfloat16 [16384, 320], P(('bev', 'scene'))
The draws below stay inside these ranges and needn't reach their ends.
Inputs may be any that keep to these rules, and one draw needn't show every extreme that they name: `send_count`: one entry is 1024 in every pixel block's row. `slot_point`: the live slots of one pixel block name distinct points; slots at or past the count are unused.
All inputs are finite; a program needn't handle non-finite values.
Results may differ from the reference program's by a relative error of at most 0.0062.
Values may be sent and summed in bfloat16 or wider, within the bound.
No kernel may reach another device: no remote copies, remote signals or barrier semaphores. Data moves between devices by JAX's collectives and lax.ppermute only.
A program may use at most 128 MiB of HBM per device.

```python
import jax
import jax.numpy as jnp
from jax import lax

C = 80
DEPTH = 112
GRID = 128
PIX_DEV = 256
STRIPS = 64
SCENES = 4
PIXELS = 16384
CAP = 1024


def draw_context(key, part):
    keys = jax.random.split(jax.random.fold_in(key, 5), 3)
    values = 4.0 * jax.random.normal(keys[2], (SCENES, C, PIXELS), jnp.float32)
    return jnp.clip(values, -24.0, 24.0).astype(jnp.bfloat16)


def draw_depth_logits(key, part):
    keys = jax.random.split(jax.random.fold_in(key, 11), 10)
    base = 0.5 * jax.random.normal(keys[9], (SCENES, DEPTH, PIXELS), jnp.float32)
    return jnp.clip(base, -3.0, 3.0).astype(jnp.float32)


def routing_tables(key):
    base_key = jax.random.fold_in(key, 7)
    strip_cells = GRID * GRID // STRIPS
    point_total = PIX_DEV * DEPTH

    def one_block(sub):
        keys = jax.random.split(sub, 6)
        window_start = jax.random.randint(keys[0], (), 0, STRIPS)
        strip_ids = jnp.arange(STRIPS, dtype=jnp.int32)
        inside = (strip_ids - window_start) % STRIPS < STRIPS // 4
        heavy = jax.random.randint(keys[1], (STRIPS,), 3 * CAP // 4, CAP + 1)
        light = jax.random.randint(keys[2], (STRIPS,), 0, CAP // 6 + 1)
        counts = jnp.where(inside, heavy, light)
        full_strip = (window_start + jax.random.randint(keys[3], (), 0, STRIPS // 4)) % STRIPS
        counts = jnp.where(strip_ids == full_strip, CAP, counts).astype(jnp.int32)
        order = jax.random.permutation(keys[4], point_total).astype(jnp.int32)
        offset = jnp.cumsum(counts) - counts
        positions = (offset[:, None] + jnp.arange(CAP, dtype=jnp.int32)[None, :]) % point_total
        points = order[positions]
        cells = jax.random.randint(keys[5], (STRIPS, CAP), 0, strip_cells)
        return (counts, points, cells)
    subkeys = jax.random.split(base_key, SCENES * STRIPS)
    counts, points, cells = jax.vmap(one_block)(subkeys)
    return (counts.reshape(SCENES, STRIPS, STRIPS), points.reshape(SCENES, STRIPS, STRIPS, CAP), cells.reshape(SCENES, STRIPS, STRIPS, CAP))


def draw_send_count(key, part):
    return routing_tables(key)[0].astype(jnp.int32)


def draw_slot_point(key, part):
    return routing_tables(key)[1].astype(jnp.int32)


def draw_slot_cell(key, part):
    return routing_tables(key)[2].astype(jnp.int32)


def setup_inputs(seed: int = 0) -> dict:
    streams_of = jax.random.split(jax.random.key(seed), 6)
    return {
        "context": draw_context(jax.random.fold_in(streams_of[5], 71), 0),
        "depth_logits": draw_depth_logits(jax.random.fold_in(streams_of[5], 71), 0),
        "send_count": draw_send_count(jax.random.fold_in(streams_of[5], 71), 0),
        "slot_point": draw_slot_point(jax.random.fold_in(streams_of[5], 71), 0),
        "slot_cell": draw_slot_cell(jax.random.fold_in(streams_of[5], 71), 0),
    }


def reference(context, depth_logits, send_count, slot_point, slot_cell):
    depth_prob = jax.nn.softmax(depth_logits.astype(jnp.float32), axis=1).astype(jnp.bfloat16)
    strip_cells = GRID * GRID // STRIPS

    def scene_sum(blocks):
        scene_ctx, scene_prob, scene_count, scene_points, scene_cells = blocks

        def add_source(running, source):
            ctx_block = lax.dynamic_slice_in_dim(scene_ctx, source * PIX_DEV, PIX_DEV, 1)
            prob_block = lax.dynamic_slice_in_dim(scene_prob, source * PIX_DEV, PIX_DEV, 1)
            point_ids = scene_points[source].reshape(-1)
            depth_bin = point_ids // PIX_DEV
            pixel_ids = point_ids % PIX_DEV
            weight = prob_block[depth_bin, pixel_ids].astype(jnp.float32)
            features = ctx_block[:, pixel_ids].T.astype(jnp.float32)
            values = (features * weight[:, None]).astype(jnp.bfloat16)
            live_mask = jnp.arange(CAP, dtype=jnp.int32)[None, :] < scene_count[source][:, None]
            strip_base = jnp.arange(STRIPS, dtype=jnp.int32)[:, None] * strip_cells
            targets = jnp.where(live_mask, strip_base + scene_cells[source], GRID * GRID).reshape(-1).astype(jnp.int32)
            pooled = jax.ops.segment_sum(values.astype(jnp.float32), targets, num_segments=GRID * GRID + 1)
            return running + pooled[:GRID * GRID], None

        running, _ = lax.scan(add_source, jnp.zeros((GRID * GRID, C), jnp.float32), jnp.arange(STRIPS, dtype=jnp.int32))
        return running

    sums = lax.map(scene_sum, (context, depth_prob, send_count, slot_point, slot_cell))
    return jnp.transpose(sums, (1, 0, 2)).reshape(GRID * GRID, SCENES * C).astype(jnp.bfloat16)
```

```python
import jax
import jax.numpy as jnp
from jax import lax
from jax.experimental import pallas as pl
from jax.experimental.pallas import tpu as pltpu
from jax.sharding import Mesh, PartitionSpec as P

C = 80
DEPTH = 112
PIX = 256
CELLS = 256
STRIPS = 64
CAP = 1024
CHUNK = 256
NCH = CAP // CHUNK
TILES = CAP // 128
GROUP = 8
ZS = 8
SLOT_ROWS = 3 * ZS * NCH
ROWS = SLOT_ROWS + C
BATCH_A = 8
BATCH_B = 4

BF = jnp.bfloat16
F32 = jnp.float32


def iota16(lanes):
    return lax.broadcasted_iota(jnp.int32, (16, lanes), 0).astype(F32).astype(BF)


def onehot_rows(row, count):
    lanes = row.shape[1]
    base = jnp.broadcast_to(row, (16, lanes)).astype(BF) - iota16(lanes)
    one, zero = jnp.ones((16, lanes), BF), jnp.zeros((16, lanes), BF)
    return jnp.concatenate(
        [jnp.where(base == jnp.asarray(16.0 * g, BF), one, zero) for g in range(count // 16)], axis=0
    )


def send_kernel(count_ref, logits_ref, ctx_ref, point_ref, cell_ref, out_ref, prob_ref, weight_ref, pixel_ref, target_ref):
    logits = logits_ref[...]
    shifted = jnp.exp(logits - jnp.max(logits, axis=0, keepdims=True))
    prob_ref[...] = (shifted / jnp.sum(shifted, axis=0, keepdims=True)).astype(BF)
    weight_ref[...] = jnp.zeros(weight_ref.shape, F32)

    def chunks_of(strip):
        inside = jnp.minimum(strip, STRIPS - 1)
        return jnp.maximum((count_ref[inside] + (CHUNK - 1)) // CHUNK, 1)

    total = lax.fori_loop(0, STRIPS, lambda d, s: s + chunks_of(d), jnp.int32(0))
    bins = lax.broadcasted_iota(jnp.int32, (DEPTH, CHUNK), 0)

    def step(_, carry):
        strip, j = carry
        for _ in range(BATCH_A):
            row = jnp.minimum(strip, STRIPS - 1)
            lane = pl.multiple_of(j * CHUNK, CHUNK)
            point = point_ref[pl.ds(row, 1), pl.ds(lane, CHUNK)]
            pixel = (point & (PIX - 1)).astype(F32)
            hot = onehot_rows(pixel, PIX)
            column = jnp.dot(prob_ref[...], hot, preferred_element_type=F32)
            bin_id = jnp.broadcast_to(point >> 8, (DEPTH, CHUNK))
            weight = jnp.sum(jnp.where(bin_id == bins, column, 0.0), axis=0, keepdims=True)
            weight_ref[2 * j, pl.ds(row, 1), :] = weight[:, :128]
            weight_ref[2 * j + 1, pl.ds(row, 1), :] = weight[:, 128:]
            last = j + 1 >= chunks_of(strip)
            strip = jnp.where(last, strip + 1, strip)
            j = jnp.where(last, 0, j + 1)
        return strip, j

    lax.fori_loop(0, (total + BATCH_A - 1) // BATCH_A, step, (jnp.int32(0), jnp.int32(0)))

    sub = lax.broadcasted_iota(jnp.int32, (GROUP, CAP), 0)
    slot = lax.broadcasted_iota(jnp.int32, (GROUP, CAP), 1)
    for z in range(ZS):
        rows = slice(z * GROUP, (z + 1) * GROUP)
        limit = jnp.zeros((GROUP, CAP), jnp.int32)
        for dest in range(GROUP):
            limit = jnp.where(sub == dest, count_ref[z * GROUP + dest], limit)
        pixel = jnp.where(slot < limit, point_ref[rows, :] & (PIX - 1), -1).astype(F32)
        cell = cell_ref[rows, :].astype(F32)
        for t in range(TILES):
            pixel_ref[t, rows, :] = pixel[:, t * 128 : (t + 1) * 128]
            target_ref[t, rows, :] = cell[:, t * 128 : (t + 1) * 128]
    context = ctx_ref[...]
    for dest in range(GROUP):
        for kind, ref in enumerate((weight_ref, pixel_ref, target_ref)):
            for half in range(2):
                stacked = jnp.concatenate(
                    [ref[2 * i + half, pl.ds(dest, ZS, stride=GROUP), :] for i in range(NCH)], axis=0
                )
                out_ref[
                    dest, kind * ZS * NCH : (kind + 1) * ZS * NCH, half * 128 : (half + 1) * 128
                ] = stacked.astype(BF)
        out_ref[dest, SLOT_ROWS:ROWS, :] = context


def pool_kernel(in_ref, out_ref, slots_ref, acc_ref, val_ref, word_ref):
    for src in range(GROUP):
        slots_ref[src * SLOT_ROWS : (src + 1) * SLOT_ROWS, :] = in_ref[src, :SLOT_ROWS, :].astype(F32)
    acc_ref[...] = jnp.zeros(acc_ref.shape, F32)
    val_ref[...] = jnp.zeros(val_ref.shape, BF)

    rows = ZS * NCH
    lane0 = lax.broadcasted_iota(jnp.int32, (ZS, 128), 1) == 0
    digit = jnp.left_shift(1, 3 * lax.broadcasted_iota(jnp.int32, (ZS, 128), 0)).astype(F32)
    total = jnp.int32(0)
    for src in range(GROUP):
        live = jnp.zeros((ZS, 128), F32)
        for j in range(NCH):
            first = slots_ref[src * SLOT_ROWS + rows + j * ZS : src * SLOT_ROWS + rows + (j + 1) * ZS, :128]
            on = first >= 0.0
            if j == 0:
                on = on | True
            live = live + jnp.where(lane0 & on, 1.0, 0.0)
        word_ref[src] = jnp.sum(live * digit).astype(jnp.int32)
        total = total + jnp.sum(live).astype(jnp.int32)
    word_ref[GROUP] = 0

    def step(it, carry):
        src, z, j = carry[:3]
        older = carry[3:]
        now, before = lax.rem(it, 2), lax.rem(it + 1, 2)
        fresh = []
        for b in range(BATCH_B):
            old_row, old_acc = older[2 * b], older[2 * b + 1]
            cell = slots_ref[pl.ds(old_row, 1), :]
            hot = onehot_rows(cell, CELLS)
            part = lax.dot_general(
                val_ref[before, b], hot, (((1,), (1,)), ((), ())), preferred_element_type=F32
            )
            acc_ref[old_acc] = acc_ref[old_acc] + part

            valid = src < GROUP
            source = jnp.where(valid, src, 0)
            row = source * SLOT_ROWS + j * ZS + z
            weight = slots_ref[pl.ds(row, 1), :]
            pixel = slots_ref[pl.ds(row + rows, 1), :]
            hot = onehot_rows(pixel, PIX)
            feature = jnp.dot(in_ref[source, SLOT_ROWS:ROWS, :], hot, preferred_element_type=F32)
            val_ref[now, b] = (feature * weight).astype(BF)
            fresh += [row + 2 * rows, jnp.where(valid, z, ZS)]

            chunks = jnp.right_shift(word_ref[jnp.minimum(src, GROUP)], 3 * z) & 7
            last = j + 1 >= chunks
            j = jnp.where(last, 0, j + 1)
            z = jnp.where(last, z + 1, z)
            wrap = z >= ZS
            z = jnp.where(wrap, 0, z)
            src = jnp.where(wrap, src + 1, src)
        return (src, z, j, *fresh)

    zero = jnp.int32(0)
    start = (zero, zero, zero) + (zero, jnp.int32(ZS)) * BATCH_B
    lax.fori_loop(0, (total + BATCH_B - 1) // BATCH_B + 1, step, start)

    left = lax.broadcasted_iota(jnp.int32, (C // 2, 128), 1) < 64
    for z in range(ZS):
        for t in range(2):
            a = acc_ref[z, : C // 2, t * 128 : (t + 1) * 128]
            b = acc_ref[z, C // 2 :, t * 128 : (t + 1) * 128]
            out_ref[z * 4 + 2 * t] = jnp.where(left, a, pltpu.roll(b, 64, 1)).astype(BF)
            out_ref[z * 4 + 2 * t + 1] = jnp.where(left, pltpu.roll(a, 64, 1), b).astype(BF)


def merge_kernel(in_ref, out_ref):
    parts = []
    for s in range(4):
        total = jnp.zeros((C // 2, 128), F32)
        for z in range(ZS):
            total = total + in_ref[z * 4 + s].astype(F32)
        parts += [total, pltpu.roll(total, 64, 1)]
    stacked = jnp.concatenate(parts, axis=0)
    out_ref[...] = stacked.T[:64, :].astype(BF)


VMEM = pl.BlockSpec(memory_space=pltpu.VMEM)
SMEM = pl.BlockSpec(memory_space=pltpu.SMEM)


def send(counts, logits, context, points, cells):
    return pl.pallas_call(
        send_kernel,
        out_shape=jax.ShapeDtypeStruct((GROUP, ROWS, PIX), BF),
        in_specs=[SMEM, VMEM, VMEM, VMEM, VMEM],
        out_specs=VMEM,
        scratch_shapes=[pltpu.VMEM((DEPTH, PIX), BF)] + [pltpu.VMEM((TILES, STRIPS, 128), F32)] * 3,
        name="send_slots",
    )(counts, logits, context, points, cells)


def pool(slots):
    return pl.pallas_call(
        pool_kernel,
        out_shape=jax.ShapeDtypeStruct((ZS * 4, C // 2, 128), BF),
        in_specs=[VMEM],
        out_specs=VMEM,
        scratch_shapes=[
            pltpu.VMEM((GROUP * SLOT_ROWS, CHUNK), F32),
            pltpu.VMEM((ZS + 1, C, CELLS), F32),
            pltpu.VMEM((2, BATCH_B, C, CHUNK), BF),
            pltpu.SMEM((GROUP + 1,), jnp.int32),
        ],
        name="pool_slots",
    )(slots)


def merge(partials):
    return pl.pallas_call(
        merge_kernel,
        out_shape=jax.ShapeDtypeStruct((64, 4 * C), BF),
        in_specs=[VMEM],
        out_specs=VMEM,
        name="merge_parts",
    )(partials)


def body(context, depth_logits, send_count, slot_point, slot_cell):
    slots = send(send_count[0, 0], depth_logits[0], context[0], slot_point[0, 0], slot_cell[0, 0])
    slots = lax.all_to_all(slots, ("x", "core"), 0, 0, tiled=True)
    partials = pool(slots)
    partials = lax.all_to_all(partials, ("z", "scene"), 0, 0, tiled=True)
    return merge(partials)


def solution(mesh):
    split = Mesh(mesh.devices.reshape(8, 4, 2, 4), ("z", "x", "core", "scene"))
    bev = ("z", "x", "core")
    return jax.shard_map(
        body,
        mesh=split,
        in_specs=(
            P("scene", None, bev),
            P("scene", None, bev),
            P("scene", bev, None),
            P("scene", bev, None, None),
            P("scene", bev, None, None),
        ),
        out_specs=P(("z", "x", "core", "scene"), None),
        check_vma=False,
    )
```

```python
import jax
import jax.numpy as jnp
from jax import lax
from jax.experimental import pallas as pl
from jax.experimental.pallas import tpu as pltpu
from jax.sharding import Mesh, PartitionSpec as P

C = 80
DEPTH = 112
PIX = 256
CELLS = 256
STRIPS = 64
CAP = 1024
CHUNK = 256
NCH = CAP // CHUNK
GROUP = 8
ZS = 8
SLOT_ROWS = 3 * ZS * NCH
ROWS = SLOT_ROWS + C
BATCH_A = 16
BATCH_B = 8

BF = jnp.bfloat16
F32 = jnp.float32


def iota16(lanes):
    return lax.broadcasted_iota(jnp.int32, (16, lanes), 0).astype(F32).astype(BF)


def onehot_rows(row, count):
    lanes = row.shape[1]
    base = jnp.broadcast_to(row, (16, lanes)).astype(BF) - iota16(lanes)
    one, zero = jnp.ones((16, lanes), BF), jnp.zeros((16, lanes), BF)
    return jnp.concatenate(
        [jnp.where(base == jnp.asarray(16.0 * g, BF), one, zero) for g in range(count // 16)], axis=0
    ).astype(jnp.float8_e4m3fn)


def send_kernel(
    count_ref, logits_hbm, ctx_hbm, point_hbm, cell_hbm, out_ref,
    logits_ref, ctx_ref, point_ref, cell_ref, prob_ref, weight_ref, pixel_ref, target_ref, sems,
):
    pairs = ((logits_hbm, logits_ref), (point_hbm, point_ref), (cell_hbm, cell_ref), (ctx_hbm, ctx_ref))
    copies = [pltpu.make_async_copy(src, dst, sems.at[i]) for i, (src, dst) in enumerate(pairs)]
    for copy in copies:
        copy.start()
    weight_ref[...] = jnp.zeros(weight_ref.shape, F32)
    pixel_ref[...] = jnp.full(pixel_ref.shape, -1.0, F32)
    target_ref[...] = jnp.zeros(target_ref.shape, F32)

    def chunks_of(strip):
        inside = jnp.minimum(strip, STRIPS - 1)
        return (count_ref[inside] + (CHUNK - 1)) // CHUNK

    total = jnp.int32(0)
    for d in range(STRIPS):
        total = total + jnp.maximum((count_ref[d] + (CHUNK - 1)) // CHUNK, 1)

    copies[0].wait()
    logits = logits_ref[...]
    shifted = jnp.exp(logits - jnp.max(logits, axis=0, keepdims=True))
    prob_ref[...] = (shifted / jnp.sum(shifted, axis=0, keepdims=True)).astype(BF)
    bins = lax.broadcasted_iota(jnp.int32, (DEPTH, CHUNK), 0)
    slot = lax.broadcasted_iota(jnp.int32, (1, CHUNK), 1)
    copies[1].wait()
    copies[2].wait()

    def step(_, carry):
        strip, j = carry
        for _ in range(BATCH_A):
            row = jnp.minimum(strip, STRIPS - 1)
            lane = pl.multiple_of(j * CHUNK, CHUNK)
            point = point_ref[pl.ds(row, 1), pl.ds(lane, CHUNK)]
            pixel = (point & (PIX - 1)).astype(F32)
            hot = onehot_rows(pixel, PIX)
            column = jnp.dot(prob_ref[...], hot, preferred_element_type=F32)
            bin_id = jnp.broadcast_to(point >> 8, (DEPTH, CHUNK))
            weight = jnp.sum(jnp.where(bin_id == bins, column, 0.0), axis=0, keepdims=True)
            pixel = jnp.where(slot + lane < count_ref[row], pixel, -1.0)
            cell = cell_ref[pl.ds(row, 1), pl.ds(lane, CHUNK)].astype(F32)
            place = (row & (GROUP - 1)) * ZS + (row >> 3)
            for ref, value in ((weight_ref, weight), (pixel_ref, pixel), (target_ref, cell)):
                ref[j, pl.ds(place, 1), :] = value
            last = j + 1 >= chunks_of(strip)
            strip = jnp.where(last, strip + 1, strip)
            j = jnp.where(last, 0, j + 1)
        return strip, j

    lax.fori_loop(0, (total + BATCH_A - 1) // BATCH_A, step, (jnp.int32(0), jnp.int32(0)))

    copies[3].wait()
    context = ctx_ref[...]
    for dest in range(GROUP):
        for kind, ref in enumerate((weight_ref, pixel_ref, target_ref)):
            stacked = jnp.concatenate([ref[i, dest * ZS : (dest + 1) * ZS, :] for i in range(NCH)], axis=0)
            out_ref[dest, kind * ZS * NCH : (kind + 1) * ZS * NCH, :] = stacked.astype(BF)
        out_ref[dest, SLOT_ROWS:ROWS, :] = context


def pool_kernel(in_ref, out_ref, slots_ref, acc_ref, val_ref, word_ref):
    for src in range(GROUP):
        slots_ref[src * SLOT_ROWS : (src + 1) * SLOT_ROWS, :] = in_ref[src, :SLOT_ROWS, :].astype(F32)
    acc_ref[...] = jnp.zeros(acc_ref.shape, F32)
    val_ref[...] = jnp.zeros(val_ref.shape, BF)

    rows = ZS * NCH
    lane0 = lax.broadcasted_iota(jnp.int32, (ZS, 128), 1) == 0
    digit = jnp.left_shift(1, 3 * lax.broadcasted_iota(jnp.int32, (ZS, 128), 0)).astype(F32)
    total = jnp.int32(0)
    for src in range(GROUP):
        live = jnp.zeros((ZS, 128), F32)
        for j in range(NCH):
            first = slots_ref[src * SLOT_ROWS + rows + j * ZS : src * SLOT_ROWS + rows + (j + 1) * ZS, :128]
            on = first >= 0.0
            if j == 0:
                on = on | True
            live = live + jnp.where(lane0 & on, 1.0, 0.0)
        word_ref[src] = jnp.sum(live * digit).astype(jnp.int32)
        total = total + jnp.sum(live).astype(jnp.int32)
    word_ref[GROUP] = 0

    def step(it, carry):
        src, z, j = carry[:3]
        older = carry[3:]
        now, before = lax.rem(it, 2), lax.rem(it + 1, 2)
        fresh = []
        for b in range(BATCH_B):
            old_row, old_acc = older[2 * b], older[2 * b + 1]
            cell = slots_ref[pl.ds(old_row, 1), :]
            hot = onehot_rows(cell, CELLS)
            part = lax.dot_general(
                val_ref[before, b], hot, (((1,), (1,)), ((), ())), preferred_element_type=F32
            )
            acc_ref[old_acc] = acc_ref[old_acc] + part

            valid = src < GROUP
            source = jnp.where(valid, src, 0)
            row = source * SLOT_ROWS + j * ZS + z
            weight = slots_ref[pl.ds(row, 1), :]
            pixel = slots_ref[pl.ds(row + rows, 1), :]
            hot = onehot_rows(pixel, PIX)
            feature = jnp.dot(in_ref[source, SLOT_ROWS:ROWS, :], hot, preferred_element_type=F32)
            val_ref[now, b] = (feature * weight).astype(BF)
            fresh += [row + 2 * rows, jnp.where(valid, z, ZS)]

            chunks = jnp.right_shift(word_ref[jnp.minimum(src, GROUP)], 3 * z) & 7
            last = j + 1 >= chunks
            j = jnp.where(last, 0, j + 1)
            z = jnp.where(last, z + 1, z)
            wrap = z >= ZS
            z = jnp.where(wrap, 0, z)
            src = jnp.where(wrap, src + 1, src)
        return (src, z, j, *fresh)

    zero = jnp.int32(0)
    start = (zero, zero, zero) + (zero, jnp.int32(ZS)) * BATCH_B
    lax.fori_loop(0, (total + BATCH_B - 1) // BATCH_B + 1, step, start)

    left = lax.broadcasted_iota(jnp.int32, (C // 2, 128), 1) < 64
    for z in range(ZS):
        for t in range(2):
            a = acc_ref[z, : C // 2, t * 128 : (t + 1) * 128]
            b = acc_ref[z, C // 2 :, t * 128 : (t + 1) * 128]
            out_ref[z * 4 + 2 * t] = jnp.where(left, a, pltpu.roll(b, 64, 1)).astype(BF)
            out_ref[z * 4 + 2 * t + 1] = jnp.where(left, pltpu.roll(a, 64, 1), b).astype(BF)


def merge_kernel(in_ref, out_ref):
    parts = []
    for s in range(4):
        total = jnp.zeros((C // 2, 128), F32)
        for z in range(ZS):
            total = total + in_ref[z * 4 + s].astype(F32)
        parts += [total, pltpu.roll(total, 64, 1)]
    stacked = jnp.concatenate(parts, axis=0)
    out_ref[...] = stacked.T[:64, :].astype(BF)


PARAMS = pltpu.CompilerParams(vmem_limit_bytes=12 * 1024 * 1024)
VMEM = pl.BlockSpec(memory_space=pltpu.VMEM)
HBM = pl.BlockSpec(memory_space=pltpu.HBM)
SMEM = pl.BlockSpec(memory_space=pltpu.SMEM)


def send(counts, logits, context, points, cells):
    return pl.pallas_call(
        send_kernel,
        out_shape=pltpu.VMEM((GROUP, ROWS, PIX), BF),
        in_specs=[SMEM, HBM, HBM, HBM, HBM],
        out_specs=VMEM,
        scratch_shapes=[
            pltpu.VMEM((DEPTH, PIX), F32),
            pltpu.VMEM((C, PIX), BF),
            pltpu.VMEM((STRIPS, CAP), jnp.int32),
            pltpu.VMEM((STRIPS, CAP), jnp.int32),
            pltpu.VMEM((DEPTH, PIX), BF),
            pltpu.VMEM((NCH, STRIPS, CHUNK), F32),
            pltpu.VMEM((NCH, STRIPS, CHUNK), F32),
            pltpu.VMEM((NCH, STRIPS, CHUNK), F32),
            pltpu.SemaphoreType.DMA((4,)),
        ],
        compiler_params=pltpu.CompilerParams(vmem_limit_bytes=67043328 - 800 * 1024),
        name="send_slots",
    )(counts, logits, context, points, cells)


def pool(slots):
    return pl.pallas_call(
        pool_kernel,
        out_shape=jax.ShapeDtypeStruct((ZS * 4, C // 2, 128), BF),
        in_specs=[VMEM],
        out_specs=VMEM,
        scratch_shapes=[
            pltpu.VMEM((GROUP * SLOT_ROWS, CHUNK), F32),
            pltpu.VMEM((ZS + 1, C, CELLS), F32),
            pltpu.VMEM((2, BATCH_B, C, CHUNK), BF),
            pltpu.SMEM((GROUP + 1,), jnp.int32),
        ],
        compiler_params=PARAMS,
        name="pool_slots",
    )(slots)


def merge(partials):
    return pl.pallas_call(
        merge_kernel,
        out_shape=jax.ShapeDtypeStruct((64, 4 * C), BF),
        in_specs=[VMEM],
        out_specs=VMEM,
        compiler_params=PARAMS,
        name="merge_parts",
    )(partials)


def body(context, depth_logits, send_count, slot_point, slot_cell):
    slots = send(send_count[0, 0], depth_logits[0], context[0], slot_point[0, 0], slot_cell[0, 0])
    slots = lax.all_to_all(slots, ("x", "core"), 0, 0, tiled=True)
    partials = pool(slots)
    partials = lax.all_to_all(partials, ("z", "scene"), 0, 0, tiled=True)
    return merge(partials)


def solution(mesh):
    split = Mesh(mesh.devices.reshape(8, 4, 2, 4), ("z", "x", "core", "scene"))
    bev = ("z", "x", "core")
    return jax.shard_map(
        body,
        mesh=split,
        in_specs=(
            P("scene", None, bev),
            P("scene", None, bev),
            P("scene", bev, None),
            P("scene", bev, None, None),
            P("scene", bev, None, None),
        ),
        out_specs=P(("z", "x", "core", "scene"), None),
        check_vma=False,
    )
```

```python
import jax
import jax.numpy as jnp
from jax import lax
from jax.experimental import pallas as pl
from jax.experimental.pallas import tpu as pltpu
from jax.sharding import Mesh, PartitionSpec as P

C = 80
DEPTH = 112
PIX = 256
CELLS = 256
STRIPS = 64
CAP = 1024
CHUNK = 256
NCH = CAP // CHUNK
GROUP = 8
ZS = 8
SLOT_ROWS = 3 * ZS * NCH
ROWS = SLOT_ROWS + C
BATCH_A = 56
BATCH_B = 28

BF = jnp.bfloat16
F32 = jnp.float32


def iota16(lanes):
    return lax.broadcasted_iota(jnp.int32, (16, lanes), 0).astype(F32).astype(BF)


def onehot_rows(row, count):
    lanes = row.shape[1]
    base = jnp.broadcast_to(row, (16, lanes)).astype(BF) - iota16(lanes)
    one, zero = jnp.ones((16, lanes), BF), jnp.zeros((16, lanes), BF)
    return jnp.concatenate(
        [jnp.where(base == jnp.asarray(16.0 * g, BF), one, zero) for g in range(count // 16)], axis=0
    ).astype(jnp.float8_e4m3fn)


def send_kernel(
    count_ref, logits_hbm, ctx_hbm, point_hbm, cell_hbm, out_ref,
    logits_ref, ctx_ref, point_ref, cell_ref, prob_ref, weight_ref, pixel_ref, target_ref, sems,
):
    pairs = ((logits_hbm, logits_ref), (point_hbm, point_ref), (cell_hbm, cell_ref), (ctx_hbm, ctx_ref))
    copies = [pltpu.make_async_copy(src, dst, sems.at[i]) for i, (src, dst) in enumerate(pairs)]
    for copy in copies:
        copy.start()
    weight_ref[...] = jnp.zeros(weight_ref.shape, F32)
    pixel_ref[...] = jnp.full(pixel_ref.shape, -1.0, F32)
    target_ref[...] = jnp.zeros(target_ref.shape, F32)

    def chunks_of(strip):
        inside = jnp.minimum(strip, STRIPS - 1)
        return jnp.right_shift(count_ref[inside] + (CHUNK - 1), 8)

    total = jnp.int32(0)
    for d in range(STRIPS):
        total = total + jnp.maximum(jnp.right_shift(count_ref[d] + (CHUNK - 1), 8), 1)

    copies[0].wait()
    logits = logits_ref[...]
    shifted = jnp.exp(logits - jnp.max(logits, axis=0, keepdims=True))
    prob_ref[...] = (shifted / jnp.sum(shifted, axis=0, keepdims=True)).astype(BF)
    sub8 = lax.broadcasted_iota(jnp.int32, (8, CHUNK), 0)
    slot = lax.broadcasted_iota(jnp.int32, (1, CHUNK), 1)
    copies[1].wait()
    copies[2].wait()

    def step(_, carry):
        strip, j = carry
        for _ in range(BATCH_A):
            row = jnp.minimum(strip, STRIPS - 1)
            lane = pl.multiple_of(j * CHUNK, CHUNK)
            point = point_ref[pl.ds(row, 1), pl.ds(lane, CHUNK)]
            pixel = (point & (PIX - 1)).astype(F32)
            hot = onehot_rows(pixel, PIX)
            column = jnp.dot(prob_ref[...], hot, preferred_element_type=F32)
            bin_id = jnp.broadcast_to(point >> 8, (8, CHUNK))
            level = [column[8 * g : 8 * g + 8, :] for g in range(DEPTH // 8)]
            for bit in (8, 16, 32, 64):
                upper = (bin_id & bit) != 0
                level = [
                    jnp.where(upper, level[i + 1], level[i]) if i + 1 < len(level) else level[i]
                    for i in range(0, len(level), 2)
                ]
            weight = jnp.sum(jnp.where((bin_id & 7) == sub8, level[0], 0.0), axis=0, keepdims=True)
            pixel = jnp.where(slot + lane < count_ref[row], pixel, -1.0)
            cell = cell_ref[pl.ds(row, 1), pl.ds(lane, CHUNK)].astype(F32)
            place = ((row >> 1) & (GROUP - 1)) * ZS + (row & 1) * (ZS // 2) + (row >> 4)
            for ref, value in ((weight_ref, weight), (pixel_ref, pixel), (target_ref, cell)):
                ref[j, pl.ds(place, 1), :] = value
            last = j + 1 >= chunks_of(strip)
            strip = jnp.where(last, strip + 1, strip)
            j = jnp.where(last, 0, j + 1)
        return strip, j

    lax.fori_loop(0, (total + BATCH_A - 1) // BATCH_A, step, (jnp.int32(0), jnp.int32(0)))

    copies[3].wait()
    context = ctx_ref[...]
    for dest in range(GROUP):
        for kind, ref in enumerate((weight_ref, pixel_ref, target_ref)):
            stacked = jnp.concatenate([ref[i, dest * ZS : (dest + 1) * ZS, :] for i in range(NCH)], axis=0)
            out_ref[dest, kind * ZS * NCH : (kind + 1) * ZS * NCH, :] = stacked.astype(BF)
        out_ref[dest, SLOT_ROWS:ROWS, :] = context


def pool_kernel(in_ref, out_ref, slots_ref, acc_ref, val_ref, word_ref):
    for src in range(GROUP):
        slots_ref[src * SLOT_ROWS : (src + 1) * SLOT_ROWS, :] = in_ref[src, :SLOT_ROWS, :].astype(F32)
    acc_ref[...] = jnp.zeros(acc_ref.shape, F32)

    rows = ZS * NCH
    lane0 = lax.broadcasted_iota(jnp.int32, (ZS, 128), 1) == 0
    digit = jnp.left_shift(1, 3 * lax.broadcasted_iota(jnp.int32, (ZS, 128), 0)).astype(F32)
    total = jnp.int32(0)
    for src in range(GROUP):
        live = jnp.zeros((ZS, 128), F32)
        for j in range(NCH):
            first = slots_ref[src * SLOT_ROWS + rows + j * ZS : src * SLOT_ROWS + rows + (j + 1) * ZS, :128]
            on = first >= 0.0
            if j == 0:
                on = on | True
            live = live + jnp.where(lane0 & on, 1.0, 0.0)
        word_ref[src] = jnp.sum(live * digit).astype(jnp.int32)
        total = total + jnp.sum(live).astype(jnp.int32)
    word_ref[GROUP] = 0

    def select(slot, b, state):
        src, z, j = state
        valid = src < GROUP
        source = jnp.where(valid, src, 0)
        row = source * SLOT_ROWS + j * ZS + z
        weight = slots_ref[pl.ds(row, 1), :]
        pixel = slots_ref[pl.ds(row + rows, 1), :]
        hot = onehot_rows(pixel, PIX)
        feature = jnp.dot(in_ref[source, SLOT_ROWS:ROWS, :], hot, preferred_element_type=F32)
        val_ref[slot, b] = (feature * weight).astype(BF)
        item = (row + 2 * rows, jnp.where(valid, z, ZS))
        chunks = jnp.right_shift(word_ref[jnp.minimum(src, GROUP)], 3 * z) & 7
        last = j + 1 >= chunks
        j = jnp.where(last, 0, j + 1)
        z = jnp.where(last, z + 1, z)
        wrap = z >= ZS
        z = jnp.where(wrap, 0, z)
        src = jnp.where(wrap, src + 1, src)
        return (src, z, j), item

    def gather(slot, b, item):
        row, place = item
        hot = onehot_rows(slots_ref[pl.ds(row, 1), :], CELLS)
        part = lax.dot_general(
            val_ref[slot, b], hot, (((1,), (1,)), ((), ())), preferred_element_type=F32
        )
        acc_ref[place] = acc_ref[place] + part

    def step(it, carry):
        state, items = carry
        before, now = lax.rem(it, 2), lax.rem(it + 1, 2)
        fresh = []
        for b in range(BATCH_B):
            gather(before, b, items[b])
            state, item = select(now, b, state)
            fresh.append(item)
        return state, tuple(fresh)

    zero = jnp.int32(0)
    batches = (total + BATCH_B - 1) // BATCH_B
    state, items = (zero, zero, zero), []
    for b in range(BATCH_B):
        state, item = select(0, b, state)
        items.append(item)
    _, items = lax.fori_loop(0, batches - 1, step, (state, tuple(items)))
    for b in range(BATCH_B):
        gather(lax.rem(batches - 1, 2), b, items[b])

    left = lax.broadcasted_iota(jnp.int32, (C // 2, 128), 1) < 64
    for z in range(ZS):
        for t in range(2):
            a = acc_ref[z, : C // 2, t * 128 : (t + 1) * 128]
            b = acc_ref[z, C // 2 :, t * 128 : (t + 1) * 128]
            out_ref[z * 4 + 2 * t] = jnp.where(left, a, pltpu.roll(b, 64, 1)).astype(BF)
            out_ref[z * 4 + 2 * t + 1] = jnp.where(left, pltpu.roll(a, 64, 1), b).astype(BF)


def merge_kernel(in_ref, out_ref):
    parts = []
    for s in range(4):
        total = jnp.zeros((C // 2, 128), F32)
        for z in range(ZS // 2):
            total = total + in_ref[z * 4 + s].astype(F32)
        parts += [total, pltpu.roll(total, 64, 1)]
    stacked = jnp.concatenate(parts, axis=0)
    out_ref[...] = stacked.T[:64, :].astype(BF)


PARAMS = pltpu.CompilerParams(vmem_limit_bytes=12 * 1024 * 1024)
VMEM = pl.BlockSpec(memory_space=pltpu.VMEM)
HBM = pl.BlockSpec(memory_space=pltpu.HBM)
SMEM = pl.BlockSpec(memory_space=pltpu.SMEM)


def send(counts, logits, context, points, cells):
    return pl.pallas_call(
        send_kernel,
        out_shape=pltpu.VMEM((GROUP, ROWS, PIX), BF),
        in_specs=[SMEM, HBM, HBM, HBM, HBM],
        out_specs=VMEM,
        scratch_shapes=[
            pltpu.VMEM((DEPTH, PIX), F32),
            pltpu.VMEM((C, PIX), BF),
            pltpu.VMEM((STRIPS, CAP), jnp.int32),
            pltpu.VMEM((STRIPS, CAP), jnp.int32),
            pltpu.VMEM((DEPTH, PIX), BF),
            pltpu.VMEM((NCH, STRIPS, CHUNK), F32),
            pltpu.VMEM((NCH, STRIPS, CHUNK), F32),
            pltpu.VMEM((NCH, STRIPS, CHUNK), F32),
            pltpu.SemaphoreType.DMA((4,)),
        ],
        compiler_params=pltpu.CompilerParams(vmem_limit_bytes=67043328 - 800 * 1024),
        name="send_slots",
    )(counts, logits, context, points, cells)


def pool(slots):
    return pl.pallas_call(
        pool_kernel,
        out_shape=jax.ShapeDtypeStruct((ZS * 4, C // 2, 128), BF),
        in_specs=[VMEM],
        out_specs=VMEM,
        scratch_shapes=[
            pltpu.VMEM((GROUP * SLOT_ROWS, CHUNK), F32),
            pltpu.VMEM((ZS + 1, C, CELLS), F32),
            pltpu.VMEM((2, BATCH_B, C, CHUNK), BF),
            pltpu.SMEM((GROUP + 1,), jnp.int32),
        ],
        compiler_params=PARAMS,
        name="pool_slots",
    )(slots)


def merge(partials):
    return pl.pallas_call(
        merge_kernel,
        out_shape=jax.ShapeDtypeStruct((64, 4 * C), BF),
        in_specs=[VMEM],
        out_specs=VMEM,
        compiler_params=PARAMS,
        name="merge_parts",
    )(partials)


def body(context, depth_logits, send_count, slot_point, slot_cell):
    slots = send(send_count[0, 0], depth_logits[0], context[0], slot_point[0, 0], slot_cell[0, 0])
    slots = lax.all_to_all(slots, ("zl", "x"), 0, 0, tiled=True)
    mine = pool(slots).reshape(2, 2 * ZS, C // 2, 128)
    theirs = lax.ppermute(mine, "core", [(0, 1), (1, 0)])
    core = lax.axis_index("core")
    half = [lax.dynamic_index_in_dim(v, core, 0, keepdims=False).astype(F32) for v in (mine, theirs)]
    partials = (half[0] + half[1]).astype(BF)
    partials = lax.all_to_all(partials, ("zh", "scene"), 0, 0, tiled=True)
    return merge(partials)


def solution(mesh):
    split = Mesh(mesh.devices.reshape(4, 2, 4, 2, 4), ("zh", "zl", "x", "core", "scene"))
    bev = ("zh", "zl", "x", "core")
    return jax.shard_map(
        body,
        mesh=split,
        in_specs=(
            P("scene", None, bev),
            P("scene", None, bev),
            P("scene", bev, None),
            P("scene", bev, None, None),
            P("scene", bev, None, None),
        ),
        out_specs=P((*bev, "scene"), None),
        check_vma=False,
    )
```

```python
import jax
import jax.numpy as jnp
from jax import lax
from jax.experimental import pallas as pl
from jax.experimental.pallas import tpu as pltpu
from jax.sharding import Mesh, PartitionSpec as P

C = 80
DEPTH = 112
PIX = 256
CELLS = 256
STRIPS = 64
CAP = 1024
CHUNK = 256
NCH = CAP // CHUNK
TILES = CAP // 128
GROUP = 8
ZS = 8
SLOT_ROWS = 3 * ZS * NCH
ROWS = SLOT_ROWS + C
BATCH_A = 50
BATCH_B = 28

BF = jnp.bfloat16
F32 = jnp.float32


def iota16(lanes):
    return lax.broadcasted_iota(jnp.int32, (16, lanes), 0).astype(F32).astype(BF)


def onehot_rows(row, count):
    lanes = row.shape[1]
    base = jnp.broadcast_to(row, (16, lanes)).astype(BF) - iota16(lanes)
    one, zero = jnp.ones((16, lanes), BF), jnp.zeros((16, lanes), BF)
    return jnp.concatenate(
        [jnp.where(base == jnp.asarray(16.0 * g, BF), one, zero) for g in range(count // 16)], axis=0
    ).astype(jnp.float8_e4m3fn)


def send_kernel(
    count_hbm, logits_hbm, ctx_hbm, point_hbm, cell_hbm, out_ref,
    count_ref, logits_ref, ctx_ref, raw_point_ref, raw_cell_ref, point_ref, cell_ref, prob_ref, weight_ref, pixel_ref, target_ref, sems,
):
    pairs = [(count_hbm, count_ref), (logits_hbm, logits_ref), (ctx_hbm, ctx_ref)]
    pairs += [(point_hbm, raw_point_ref), (cell_hbm, raw_cell_ref)]
    copies = [pltpu.make_async_copy(src, dst, sems.at[i]) for i, (src, dst) in enumerate(pairs)]
    for copy in copies:
        copy.start()
    weight_ref[...] = jnp.zeros(weight_ref.shape, F32)
    pixel_ref[...] = jnp.full(pixel_ref.shape, -1.0, F32)
    target_ref[...] = jnp.zeros(target_ref.shape, F32)

    def pieces_of(count):
        return jnp.maximum(jnp.right_shift(count + 127, 7), 1)

    copies[0].wait()
    total = jnp.int32(0)
    for d in range(STRIPS):
        total = total + pieces_of(count_ref[d])

    copies[1].wait()
    logits = logits_ref[...]
    shifted = jnp.exp(logits - jnp.max(logits, axis=0, keepdims=True))
    prob_ref[...] = (shifted / jnp.sum(shifted, axis=0, keepdims=True)).astype(BF)
    sub8 = lax.broadcasted_iota(jnp.int32, (8, 128), 0)
    slot = lax.broadcasted_iota(jnp.int32, (1, 128), 1)
    for copy in copies[2:]:
        copy.wait()
    for t in range(TILES):
        point_ref[t] = raw_point_ref[:, t * 128 : (t + 1) * 128]
        cell_ref[t] = raw_cell_ref[:, t * 128 : (t + 1) * 128]

    def step(_, carry):
        strip, j = carry
        for _ in range(BATCH_A):
            rows, hots = [], []
            for _ in range(2):
                row = jnp.minimum(strip, STRIPS - 1)
                count = count_ref[row]
                point = point_ref[j, pl.ds(row, 1), :]
                rows.append((row, j, count, point))
                hots.append(onehot_rows((point & (PIX - 1)).astype(F32), PIX))
                last = j + 1 >= pieces_of(count)
                strip = jnp.where(last, strip + 1, strip)
                j = jnp.where(last, 0, j + 1)
            hot = jnp.concatenate(hots, axis=1)
            columns = jnp.dot(prob_ref[...], hot, preferred_element_type=F32)
            for half, (row, piece, count, point) in enumerate(rows):
                bin_id = jnp.broadcast_to(jnp.right_shift(point, 8), (8, 128))
                column = columns[:, half * 128 : (half + 1) * 128]
                level = [column[8 * g : 8 * g + 8, :] for g in range(DEPTH // 8)]
                for bit in (8, 16, 32, 64):
                    upper = (bin_id & bit) != 0
                    level = [
                        jnp.where(upper, level[i + 1], level[i]) if i + 1 < len(level) else level[i]
                        for i in range(0, len(level), 2)
                    ]
                weight = jnp.sum(jnp.where((bin_id & 7) == sub8, level[0], 0.0), axis=0, keepdims=True)
                pixel = jnp.where(slot + piece * 128 < count, point & (PIX - 1), -1).astype(F32)
                cell = cell_ref[piece, pl.ds(row, 1), :].astype(F32)
                inside = jnp.right_shift(row, 1)
                place = (inside & (GROUP - 1)) * ZS + (row & 1) * (ZS // 2) + jnp.right_shift(row, 4)
                for ref, value in ((weight_ref, weight), (pixel_ref, pixel), (target_ref, cell)):
                    ref[piece, pl.ds(place, 1), :] = value
        return strip, j

    steps = (total + 2 * BATCH_A - 1) // (2 * BATCH_A)
    lax.fori_loop(0, steps, step, (jnp.int32(0), jnp.int32(0)))

    context = ctx_ref[...]
    for dest in range(GROUP):
        for kind, ref in enumerate((weight_ref, pixel_ref, target_ref)):
            for half in range(2):
                stacked = jnp.concatenate(
                    [ref[2 * i + half, dest * ZS : (dest + 1) * ZS, :] for i in range(NCH)], axis=0
                )
                out_ref[
                    dest, kind * ZS * NCH : (kind + 1) * ZS * NCH, half * 128 : (half + 1) * 128
                ] = stacked.astype(BF)
        out_ref[dest, SLOT_ROWS:ROWS, :] = context


def pool_kernel(in_ref, out_ref, slots_ref, acc_ref, val_ref, word_ref):
    for src in range(GROUP):
        slots_ref[src * SLOT_ROWS : (src + 1) * SLOT_ROWS, :] = in_ref[src, :SLOT_ROWS, :].astype(F32)
    acc_ref[...] = jnp.zeros(acc_ref.shape, F32)

    rows = ZS * NCH
    lane0 = lax.broadcasted_iota(jnp.int32, (ZS, 128), 1) == 0
    digit = jnp.left_shift(1, 3 * lax.broadcasted_iota(jnp.int32, (ZS, 128), 0)).astype(F32)
    total = jnp.int32(0)
    for src in range(GROUP):
        live = jnp.zeros((ZS, 128), F32)
        for j in range(NCH):
            first = slots_ref[src * SLOT_ROWS + rows + j * ZS : src * SLOT_ROWS + rows + (j + 1) * ZS, :128]
            on = first >= 0.0
            if j == 0:
                on = on | True
            live = live + jnp.where(lane0 & on, 1.0, 0.0)
        word_ref[src] = jnp.sum(live * digit).astype(jnp.int32)
        total = total + jnp.sum(live).astype(jnp.int32)
    word_ref[GROUP] = 0

    def select(slot, b, state):
        src, z, j = state
        valid = src < GROUP
        source = jnp.where(valid, src, 0)
        row = source * SLOT_ROWS + j * ZS + z
        weight = slots_ref[pl.ds(row, 1), :]
        pixel = slots_ref[pl.ds(row + rows, 1), :]
        hot = onehot_rows(pixel, PIX)
        feature = jnp.dot(in_ref[source, SLOT_ROWS:ROWS, :], hot, preferred_element_type=F32)
        val_ref[slot, b] = (feature * weight).astype(BF)
        item = (row + 2 * rows, jnp.where(valid, z, ZS))
        chunks = jnp.right_shift(word_ref[jnp.minimum(src, GROUP)], 3 * z) & 7
        last = j + 1 >= chunks
        j = jnp.where(last, 0, j + 1)
        z = jnp.where(last, z + 1, z)
        wrap = z >= ZS
        z = jnp.where(wrap, 0, z)
        src = jnp.where(wrap, src + 1, src)
        return (src, z, j), item

    def gather(slot, b, item):
        row, place = item
        hot = onehot_rows(slots_ref[pl.ds(row, 1), :], CELLS)
        part = lax.dot_general(
            val_ref[slot, b], hot, (((1,), (1,)), ((), ())), preferred_element_type=F32
        )
        acc_ref[place] = acc_ref[place] + part

    def step(it, carry):
        state, items = carry
        before, now = lax.rem(it, 2), lax.rem(it + 1, 2)
        fresh = []
        for b in range(BATCH_B):
            gather(before, b, items[b])
            state, item = select(now, b, state)
            fresh.append(item)
        return state, tuple(fresh)

    zero = jnp.int32(0)
    batches = (total + BATCH_B - 1) // BATCH_B
    state, items = (zero, zero, zero), []
    for b in range(BATCH_B):
        state, item = select(0, b, state)
        items.append(item)
    _, items = lax.fori_loop(0, batches - 1, step, (state, tuple(items)))
    for b in range(BATCH_B):
        gather(lax.rem(batches - 1, 2), b, items[b])

    left = lax.broadcasted_iota(jnp.int32, (C // 2, 128), 1) < 64
    for z in range(ZS):
        for t in range(2):
            a = acc_ref[z, : C // 2, t * 128 : (t + 1) * 128]
            b = acc_ref[z, C // 2 :, t * 128 : (t + 1) * 128]
            out_ref[z * 4 + 2 * t] = jnp.where(left, a, pltpu.roll(b, 64, 1)).astype(BF)
            out_ref[z * 4 + 2 * t + 1] = jnp.where(left, pltpu.roll(a, 64, 1), b).astype(BF)


def merge_kernel(in_ref, out_ref):
    parts = []
    for s in range(4):
        total = jnp.zeros((C // 2, 128), F32)
        for z in range(ZS // 2):
            total = total + in_ref[z * 4 + s].astype(F32)
        parts += [total, pltpu.roll(total, 64, 1)]
    stacked = jnp.concatenate(parts, axis=0)
    out_ref[...] = stacked.T[:64, :].astype(BF)


PARAMS = pltpu.CompilerParams(vmem_limit_bytes=12 * 1024 * 1024)
VMEM = pl.BlockSpec(memory_space=pltpu.VMEM)
HBM = pl.BlockSpec(memory_space=pltpu.HBM)
SMEM = pl.BlockSpec(memory_space=pltpu.SMEM)


def send(counts, logits, context, points, cells):
    return pl.pallas_call(
        send_kernel,
        out_shape=pltpu.VMEM((GROUP, ROWS, PIX), BF),
        in_specs=[HBM, HBM, HBM, HBM, HBM],
        out_specs=VMEM,
        scratch_shapes=[
            pltpu.SMEM((STRIPS,), jnp.int32),
            pltpu.VMEM((DEPTH, PIX), F32),
            pltpu.VMEM((C, PIX), BF),
            pltpu.VMEM((STRIPS, CAP), jnp.int32),
            pltpu.VMEM((STRIPS, CAP), jnp.int32),
            pltpu.VMEM((TILES, STRIPS, 128), jnp.int32),
            pltpu.VMEM((TILES, STRIPS, 128), jnp.int32),
            pltpu.VMEM((DEPTH, PIX), BF),
            pltpu.VMEM((TILES, STRIPS, 128), F32),
            pltpu.VMEM((TILES, STRIPS, 128), F32),
            pltpu.VMEM((TILES, STRIPS, 128), F32),
            pltpu.SemaphoreType.DMA((5,)),
        ],
        compiler_params=pltpu.CompilerParams(vmem_limit_bytes=67043328 - 800 * 1024),
        name="send_slots",
    )(counts, logits, context, points, cells)


def pool(slots):
    return pl.pallas_call(
        pool_kernel,
        out_shape=jax.ShapeDtypeStruct((ZS * 4, C // 2, 128), BF),
        in_specs=[VMEM],
        out_specs=VMEM,
        scratch_shapes=[
            pltpu.VMEM((GROUP * SLOT_ROWS, CHUNK), F32),
            pltpu.VMEM((ZS + 1, C, CELLS), F32),
            pltpu.VMEM((2, BATCH_B, C, CHUNK), BF),
            pltpu.SMEM((GROUP + 1,), jnp.int32),
        ],
        compiler_params=PARAMS,
        name="pool_slots",
    )(slots)


def merge(partials):
    return pl.pallas_call(
        merge_kernel,
        out_shape=jax.ShapeDtypeStruct((64, 4 * C), BF),
        in_specs=[VMEM],
        out_specs=VMEM,
        compiler_params=PARAMS,
        name="merge_parts",
    )(partials)


def body(context, depth_logits, send_count, slot_point, slot_cell):
    slots = send(send_count[0, 0], depth_logits[0], context[0], slot_point[0, 0], slot_cell[0, 0])
    slots = lax.all_to_all(slots, ("zl", "x"), 0, 0, tiled=True)
    mine = pool(slots).reshape(2, 2 * ZS, C // 2, 128)
    theirs = lax.ppermute(mine, "core", [(0, 1), (1, 0)])
    core = lax.axis_index("core")
    half = [lax.dynamic_index_in_dim(v, core, 0, keepdims=False).astype(F32) for v in (mine, theirs)]
    partials = (half[0] + half[1]).astype(BF)
    partials = lax.all_to_all(partials, ("zh", "scene"), 0, 0, tiled=True)
    return merge(partials)


def solution(mesh):
    split = Mesh(mesh.devices.reshape(4, 2, 4, 2, 4), ("zh", "zl", "x", "core", "scene"))
    bev = ("zh", "zl", "x", "core")
    return jax.shard_map(
        body,
        mesh=split,
        in_specs=(
            P("scene", None, bev),
            P("scene", None, bev),
            P("scene", bev, None),
            P("scene", bev, None, None),
            P("scene", bev, None, None),
        ),
        out_specs=P((*bev, "scene"), None),
        check_vma=False,
    )
```

```python
import functools

import jax
import jax.numpy as jnp
from jax import lax
from jax.experimental import pallas as pl
from jax.experimental.pallas import tpu as pltpu
from jax.sharding import Mesh, PartitionSpec as P

C = 80
DEPTH = 112
PIX = 256
CELLS = 256
STRIPS = 64
CAP = 1024
CHUNK = 256
NCH = CAP // CHUNK
TILES = CAP // 128
GROUP = 8
ZS = 8
SLOT_ROWS = 3 * ZS * NCH
ROWS = SLOT_ROWS + C
BATCH_A = 44
BATCH_B = 25
BATCH_OWN = 7

BF = jnp.bfloat16
F32 = jnp.float32


def iota16(lanes):
    return lax.broadcasted_iota(jnp.int32, (16, lanes), 0).astype(F32).astype(BF)


def onehot_rows(row, count):
    lanes = row.shape[1]
    base = jnp.broadcast_to(row, (16, lanes)).astype(BF) - iota16(lanes)
    one, zero = jnp.ones((16, lanes), BF), jnp.zeros((16, lanes), BF)
    return jnp.concatenate(
        [jnp.where(base == jnp.asarray(16.0 * g, BF), one, zero) for g in range(count // 16)], axis=0
    ).astype(jnp.float8_e4m3fn)


def own_place():
    return lax.axis_index(("zl", "x"))


def send_kernel(
    peers, count_hbm, logits_hbm, ctx_hbm, point_hbm, cell_hbm, out_ref,
    count_ref, logits_ref, ctx_ref, raw_point_ref, raw_cell_ref, point_ref, cell_ref, prob_ref, weight_ref, pixel_ref, target_ref, sems,
):
    pairs = [(count_hbm, count_ref), (logits_hbm, logits_ref), (ctx_hbm, ctx_ref)]
    pairs += [(point_hbm, raw_point_ref), (cell_hbm, raw_cell_ref)]
    copies = [pltpu.make_async_copy(src, dst, sems.at[i]) for i, (src, dst) in enumerate(pairs)]
    for copy in copies:
        copy.start()
    weight_ref[...] = jnp.zeros(weight_ref.shape, F32)
    pixel_ref[...] = jnp.full(pixel_ref.shape, -1.0, F32)
    target_ref[...] = jnp.zeros(target_ref.shape, F32)

    def pieces_of(count):
        return jnp.maximum(jnp.right_shift(count + 127, 7), 1)

    own = own_place()
    first = 1 if peers > 1 else 0
    strips = peers * ZS

    def row_of(strip):
        dest = (own + first + jnp.right_shift(strip, 3)) & (GROUP - 1)
        return jnp.left_shift(strip & 3, 4) + 2 * dest + (jnp.right_shift(strip, 2) & 1)

    copies[0].wait()
    total = jnp.int32(0)
    for d in range(strips):
        total = total + pieces_of(count_ref[row_of(jnp.int32(d))])

    copies[1].wait()
    logits = logits_ref[...]
    shifted = jnp.exp(logits - jnp.max(logits, axis=0, keepdims=True))
    prob_ref[...] = (shifted / jnp.sum(shifted, axis=0, keepdims=True)).astype(BF)
    sub8 = lax.broadcasted_iota(jnp.int32, (8, 128), 0)
    slot = lax.broadcasted_iota(jnp.int32, (1, 128), 1)
    for copy in copies[2:]:
        copy.wait()
    for t in range(TILES):
        point_ref[t] = raw_point_ref[:, t * 128 : (t + 1) * 128]
        cell_ref[t] = raw_cell_ref[:, t * 128 : (t + 1) * 128]

    def step(_, carry):
        strip, j = carry
        for _ in range(BATCH_A if peers > 1 else BATCH_OWN):
            rows, hots = [], []
            for _ in range(2):
                row = row_of(jnp.minimum(strip, strips - 1))
                count = count_ref[row]
                point = point_ref[j, pl.ds(row, 1), :]
                rows.append((row, j, count, point))
                hots.append(onehot_rows((point & (PIX - 1)).astype(F32), PIX))
                last = j + 1 >= pieces_of(count)
                strip = jnp.where(last, strip + 1, strip)
                j = jnp.where(last, 0, j + 1)
            hot = jnp.concatenate(hots, axis=1)
            columns = jnp.dot(prob_ref[...], hot, preferred_element_type=F32)
            for half, (row, piece, count, point) in enumerate(rows):
                bin_id = jnp.broadcast_to(jnp.right_shift(point, 8), (8, 128))
                column = columns[:, half * 128 : (half + 1) * 128]
                level = [column[8 * g : 8 * g + 8, :] for g in range(DEPTH // 8)]
                for bit in (8, 16, 32, 64):
                    upper = (bin_id & bit) != 0
                    level = [
                        jnp.where(upper, level[i + 1], level[i]) if i + 1 < len(level) else level[i]
                        for i in range(0, len(level), 2)
                    ]
                weight = jnp.sum(jnp.where((bin_id & 7) == sub8, level[0], 0.0), axis=0, keepdims=True)
                pixel = jnp.where(slot + piece * 128 < count, point & (PIX - 1), -1).astype(F32)
                cell = cell_ref[piece, pl.ds(row, 1), :].astype(F32)
                inside = jnp.right_shift(row, 1)
                place = (row & 1) * (ZS // 2) + jnp.right_shift(row, 4)
                if peers > 1:
                    place = place + (inside & (GROUP - 1)) * ZS
                for ref, value in ((weight_ref, weight), (pixel_ref, pixel), (target_ref, cell)):
                    ref[piece, pl.ds(place, 1), :] = value
        return strip, j

    batch = 2 * (BATCH_A if peers > 1 else BATCH_OWN)
    steps = (total + batch - 1) // batch
    lax.fori_loop(0, steps, step, (jnp.int32(0), jnp.int32(0)))

    context = ctx_ref[...]
    for dest in range(GROUP if peers > 1 else 1):
        for kind, ref in enumerate((weight_ref, pixel_ref, target_ref)):
            for half in range(2):
                stacked = jnp.concatenate(
                    [ref[2 * i + half, dest * ZS : (dest + 1) * ZS, :] for i in range(NCH)], axis=0
                )
                out_ref[
                    dest, kind * ZS * NCH : (kind + 1) * ZS * NCH, half * 128 : (half + 1) * 128
                ] = stacked.astype(BF)
        out_ref[dest, SLOT_ROWS:ROWS, :] = context


def pool_kernel(in_ref, *refs):
    peers = in_ref.shape[0]
    if peers > 1:
        seed_ref, out_ref, slots_ref, acc_ref, val_ref, word_ref = refs
        acc_ref[...] = seed_ref[...]
        batch = BATCH_B
    else:
        acc_ref, slots_ref, val_ref, word_ref = refs
        acc_ref[...] = jnp.zeros(acc_ref.shape, F32)
        batch = BATCH_OWN
    own = own_place()
    used = GROUP - 1 if peers > 1 else 1
    for src in range(peers):
        slots_ref[src * SLOT_ROWS : (src + 1) * SLOT_ROWS, :] = in_ref[src, :SLOT_ROWS, :].astype(F32)

    rows = ZS * NCH
    lane0 = lax.broadcasted_iota(jnp.int32, (ZS, 128), 1) == 0
    digit = jnp.left_shift(1, 3 * lax.broadcasted_iota(jnp.int32, (ZS, 128), 0)).astype(F32)
    total = jnp.int32(0)
    for src in range(peers):
        live = jnp.zeros((ZS, 128), F32)
        for j in range(NCH):
            first = slots_ref[src * SLOT_ROWS + rows + j * ZS : src * SLOT_ROWS + rows + (j + 1) * ZS, :128]
            on = first >= 0.0
            if j == 0:
                on = on | True
            live = live + jnp.where(lane0 & on, 1.0, 0.0)
        word_ref[src] = jnp.sum(live * digit).astype(jnp.int32)
        total = total + jnp.sum(live).astype(jnp.int32)
    if peers > 1:
        total = total - ZS

    def select(slot, b, state):
        src, z, j = state
        valid = src < used
        source = jnp.where(valid, src, 0)
        if peers > 1:
            source = (own + 1 + source) & (GROUP - 1)
        row = source * SLOT_ROWS + j * ZS + z
        weight = slots_ref[pl.ds(row, 1), :]
        pixel = slots_ref[pl.ds(row + rows, 1), :]
        hot = onehot_rows(pixel, PIX)
        feature = jnp.dot(in_ref[source, SLOT_ROWS:ROWS, :], hot, preferred_element_type=F32)
        val_ref[slot, b] = (feature * weight).astype(BF)
        item = (row + 2 * rows, jnp.where(valid, z, ZS))
        chunks = jnp.right_shift(word_ref[source], 3 * z) & 7
        last = j + 1 >= chunks
        j = jnp.where(last, 0, j + 1)
        z = jnp.where(last, z + 1, z)
        wrap = z >= ZS
        z = jnp.where(wrap, 0, z)
        src = jnp.where(wrap, src + 1, src)
        return (src, z, j), item

    def gather(slot, b, item):
        row, place = item
        hot = onehot_rows(slots_ref[pl.ds(row, 1), :], CELLS)
        part = lax.dot_general(
            val_ref[slot, b], hot, (((1,), (1,)), ((), ())), preferred_element_type=F32
        )
        acc_ref[place] = acc_ref[place] + part

    def step(it, carry):
        state, items = carry
        before, now = lax.rem(it, 2), lax.rem(it + 1, 2)
        fresh = []
        for b in range(batch):
            gather(before, b, items[b])
            state, item = select(now, b, state)
            fresh.append(item)
        return state, tuple(fresh)

    zero = jnp.int32(0)
    batches = (total + batch - 1) // batch
    state, items = (zero, zero, zero), []
    for b in range(batch):
        state, item = select(0, b, state)
        items.append(item)
    _, items = lax.fori_loop(0, batches - 1, step, (state, tuple(items)))
    for b in range(batch):
        gather(lax.rem(batches - 1, 2), b, items[b])

    if peers == 1:
        return
    left = lax.broadcasted_iota(jnp.int32, (C // 2, 128), 1) < 64
    for z in range(ZS):
        for t in range(2):
            a = acc_ref[z, : C // 2, t * 128 : (t + 1) * 128]
            b = acc_ref[z, C // 2 :, t * 128 : (t + 1) * 128]
            out_ref[z * 4 + 2 * t] = jnp.where(left, a, pltpu.roll(b, 64, 1)).astype(BF)
            out_ref[z * 4 + 2 * t + 1] = jnp.where(left, pltpu.roll(a, 64, 1), b).astype(BF)


def merge_kernel(in_ref, out_ref):
    parts = []
    for s in range(4):
        total = jnp.zeros((C // 2, 128), F32)
        for z in range(ZS // 2):
            total = total + in_ref[z * 4 + s].astype(F32)
        parts += [total, pltpu.roll(total, 64, 1)]
    stacked = jnp.concatenate(parts, axis=0)
    out_ref[...] = stacked.T[:64, :].astype(BF)


SEND_LIMIT = 67043328 - 3 * 1024 * 1024
PARAMS = pltpu.CompilerParams(vmem_limit_bytes=12 * 1024 * 1024)
VMEM = pl.BlockSpec(memory_space=pltpu.VMEM)
HBM = pl.BlockSpec(memory_space=pltpu.HBM)
SMEM = pl.BlockSpec(memory_space=pltpu.SMEM)


COST = pl.CostEstimate(flops=2 * 10**9, bytes_accessed=10**6, transcendentals=0)


def send(peers, counts, logits, context, points, cells):
    dests = GROUP if peers > 1 else 1
    return pl.pallas_call(
        functools.partial(send_kernel, peers),
        out_shape=pltpu.VMEM((dests, ROWS, PIX), BF),
        in_specs=[HBM, HBM, HBM, HBM, HBM],
        out_specs=VMEM,
        scratch_shapes=[
            pltpu.SMEM((STRIPS,), jnp.int32),
            pltpu.VMEM((DEPTH, PIX), F32),
            pltpu.VMEM((C, PIX), BF),
            pltpu.VMEM((STRIPS, CAP), jnp.int32),
            pltpu.VMEM((STRIPS, CAP), jnp.int32),
            pltpu.VMEM((TILES, STRIPS, 128), jnp.int32),
            pltpu.VMEM((TILES, STRIPS, 128), jnp.int32),
            pltpu.VMEM((DEPTH, PIX), BF),
            pltpu.VMEM((TILES, dests * ZS, 128), F32),
            pltpu.VMEM((TILES, dests * ZS, 128), F32),
            pltpu.VMEM((TILES, dests * ZS, 128), F32),
            pltpu.SemaphoreType.DMA((5,)),
        ],
        compiler_params=pltpu.CompilerParams(vmem_limit_bytes=SEND_LIMIT),
        cost_estimate=COST,
        name="send_slots",
    )(counts, logits, context, points, cells)


def pool(slots, *seed):
    peers = slots.shape[0]
    batch = BATCH_B if seed else BATCH_OWN
    sums = (ZS + 1, C, CELLS)
    scratch = [pltpu.VMEM((peers * SLOT_ROWS, CHUNK), F32)]
    if seed:
        scratch.append(pltpu.VMEM(sums, F32))
    return pl.pallas_call(
        pool_kernel,
        out_shape=jax.ShapeDtypeStruct((ZS * 4, C // 2, 128), BF) if seed else jax.ShapeDtypeStruct(sums, F32),
        in_specs=[VMEM] * (1 + len(seed)),
        out_specs=VMEM,
        scratch_shapes=scratch
        + [pltpu.VMEM((2, batch, C, CHUNK), BF), pltpu.SMEM((GROUP + 1,), jnp.int32)],
        compiler_params=PARAMS,
        cost_estimate=COST,
        name="pool_slots",
    )(slots, *seed)


def merge(partials):
    return pl.pallas_call(
        merge_kernel,
        out_shape=jax.ShapeDtypeStruct((64, 4 * C), BF),
        in_specs=[VMEM],
        out_specs=VMEM,
        compiler_params=PARAMS,
        name="merge_parts",
    )(partials)


def body(context, depth_logits, send_count, slot_point, slot_cell):
    block = (send_count[0, 0], depth_logits[0], context[0], slot_point[0, 0], slot_cell[0, 0])
    slots = lax.all_to_all(send(GROUP - 1, *block), ("zl", "x"), 0, 0, tiled=True)
    seed = pool(send(1, *block))
    mine = pool(slots, seed).reshape(2, 2 * ZS, C // 2, 128)
    theirs = lax.ppermute(mine, "core", [(0, 1), (1, 0)])
    core = lax.axis_index("core")
    half = [lax.dynamic_index_in_dim(v, core, 0, keepdims=False).astype(F32) for v in (mine, theirs)]
    partials = (half[0] + half[1]).astype(BF)
    partials = lax.all_to_all(partials, ("zh", "scene"), 0, 0, tiled=True)
    return merge(partials)


def solution(mesh):
    split = Mesh(mesh.devices.reshape(4, 2, 4, 2, 4), ("zh", "zl", "x", "core", "scene"))
    bev = ("zh", "zl", "x", "core")
    return jax.shard_map(
        body,
        mesh=split,
        in_specs=(
            P("scene", None, bev),
            P("scene", None, bev),
            P("scene", bev, None),
            P("scene", bev, None, None),
            P("scene", bev, None, None),
        ),
        out_specs=P((*bev, "scene"), None),
        check_vma=False,
    )
```

```python
import jax
import jax.numpy as jnp
from jax import lax
from jax.experimental import pallas as pl
from jax.experimental.pallas import tpu as pltpu
from jax.sharding import Mesh, PartitionSpec as P

C = 80
DEPTH = 112
PIX = 256
CELLS = 256
STRIPS = 64
CAP = 1024
CHUNK = 256
NCH = CAP // CHUNK
TILES = CAP // 128
GROUP = 8
ZS = 8
SLOT_ROWS = 3 * ZS * NCH
ROWS = SLOT_ROWS + C
BATCH_A = 50
BATCH_B = 28

BF = jnp.bfloat16
F32 = jnp.float32


def iota16(lanes):
    return lax.broadcasted_iota(jnp.int32, (16, lanes), 0).astype(F32).astype(BF)


def onehot_rows(row, count):
    lanes = row.shape[1]
    base = jnp.broadcast_to(row, (16, lanes)).astype(BF) - iota16(lanes)
    one, zero = jnp.ones((16, lanes), BF), jnp.zeros((16, lanes), BF)
    return jnp.concatenate(
        [jnp.where(base == jnp.asarray(16.0 * g, BF), one, zero) for g in range(count // 16)], axis=0
    ).astype(jnp.float8_e4m3fn)


def send_kernel(
    count_hbm, logits_hbm, ctx_hbm, point_hbm, cell_hbm, out_ref,
    count_ref, logits_ref, ctx_ref, raw_point_ref, raw_cell_ref, point_ref, cell_ref, prob_ref, weight_ref, pixel_ref, target_ref, sems,
):
    pairs = [(count_hbm, count_ref), (logits_hbm, logits_ref), (ctx_hbm, ctx_ref)]
    pairs += [(point_hbm, raw_point_ref), (cell_hbm, raw_cell_ref)]
    copies = [pltpu.make_async_copy(src, dst, sems.at[i]) for i, (src, dst) in enumerate(pairs)]
    for copy in copies:
        copy.start()
    weight_ref[...] = jnp.zeros(weight_ref.shape, F32)
    pixel_ref[...] = jnp.full(pixel_ref.shape, -1.0, F32)
    target_ref[...] = jnp.zeros(target_ref.shape, F32)

    def pieces_of(count):
        return jnp.maximum(jnp.right_shift(count + 127, 7), 1)

    copies[0].wait()
    total = jnp.int32(0)
    for d in range(STRIPS):
        total = total + pieces_of(count_ref[d])

    copies[1].wait()
    logits = logits_ref[...]
    shifted = jnp.exp(logits - jnp.max(logits, axis=0, keepdims=True))
    prob_ref[...] = (shifted / jnp.sum(shifted, axis=0, keepdims=True)).astype(BF)
    sub8 = lax.broadcasted_iota(jnp.int32, (8, 128), 0)
    slot = lax.broadcasted_iota(jnp.int32, (1, 128), 1)
    for copy in copies[2:]:
        copy.wait()
    for t in range(TILES):
        point_ref[t] = raw_point_ref[:, t * 128 : (t + 1) * 128]
        cell_ref[t] = raw_cell_ref[:, t * 128 : (t + 1) * 128]

    def step(_, carry):
        strip, j = carry
        for _ in range(BATCH_A):
            rows, hots = [], []
            for _ in range(2):
                row = jnp.minimum(strip, STRIPS - 1)
                count = count_ref[row]
                point = point_ref[j, pl.ds(row, 1), :]
                rows.append((row, j, count, point))
                hots.append(onehot_rows((point & (PIX - 1)).astype(F32), PIX))
                last = j + 1 >= pieces_of(count)
                strip = jnp.where(last, strip + 1, strip)
                j = jnp.where(last, 0, j + 1)
            hot = jnp.concatenate(hots, axis=1)
            columns = jnp.dot(prob_ref[...], hot, preferred_element_type=F32)
            for half, (row, piece, count, point) in enumerate(rows):
                bin_id = jnp.broadcast_to(jnp.right_shift(point, 8), (8, 128))
                column = columns[:, half * 128 : (half + 1) * 128]
                level = [column[8 * g : 8 * g + 8, :] for g in range(DEPTH // 8)]
                for bit in (8, 16, 32, 64):
                    upper = (bin_id & bit) != 0
                    level = [
                        jnp.where(upper, level[i + 1], level[i]) if i + 1 < len(level) else level[i]
                        for i in range(0, len(level), 2)
                    ]
                weight = jnp.sum(jnp.where((bin_id & 7) == sub8, level[0], 0.0), axis=0, keepdims=True)
                pixel = jnp.where(slot + piece * 128 < count, point & (PIX - 1), -1).astype(F32)
                cell = cell_ref[piece, pl.ds(row, 1), :].astype(F32)
                inside = jnp.right_shift(row, 1)
                place = (inside & (GROUP - 1)) * ZS + (row & 1) * (ZS // 2) + jnp.right_shift(row, 4)
                for ref, value in ((weight_ref, weight), (pixel_ref, pixel), (target_ref, cell)):
                    ref[piece, pl.ds(place, 1), :] = value
        return strip, j

    steps = (total + 2 * BATCH_A - 1) // (2 * BATCH_A)
    lax.fori_loop(0, steps, step, (jnp.int32(0), jnp.int32(0)))

    context = ctx_ref[...]
    for dest in range(GROUP):
        for kind, ref in enumerate((weight_ref, pixel_ref, target_ref)):
            for half in range(2):
                stacked = jnp.concatenate(
                    [ref[2 * i + half, dest * ZS : (dest + 1) * ZS, :] for i in range(NCH)], axis=0
                )
                out_ref[
                    dest, kind * ZS * NCH : (kind + 1) * ZS * NCH, half * 128 : (half + 1) * 128
                ] = stacked.astype(BF)
        out_ref[dest, SLOT_ROWS:ROWS, :] = context


def own_core():
    return lax.axis_index("core")


def pool_kernel(in_ref, mine_ref, away_ref, slots_ref, acc_ref, val_ref, word_ref):
    for src in range(GROUP):
        slots_ref[src * SLOT_ROWS : (src + 1) * SLOT_ROWS, :] = in_ref[src, :SLOT_ROWS, :].astype(F32)
    acc_ref[...] = jnp.zeros(acc_ref.shape, F32)

    rows = ZS * NCH
    lane0 = lax.broadcasted_iota(jnp.int32, (ZS, 128), 1) == 0
    digit = jnp.left_shift(1, 3 * lax.broadcasted_iota(jnp.int32, (ZS, 128), 0)).astype(F32)
    total = jnp.int32(0)
    for src in range(GROUP):
        live = jnp.zeros((ZS, 128), F32)
        for j in range(NCH):
            first = slots_ref[src * SLOT_ROWS + rows + j * ZS : src * SLOT_ROWS + rows + (j + 1) * ZS, :128]
            on = first >= 0.0
            if j == 0:
                on = on | True
            live = live + jnp.where(lane0 & on, 1.0, 0.0)
        word_ref[src] = jnp.sum(live * digit).astype(jnp.int32)
        total = total + jnp.sum(live).astype(jnp.int32)
    word_ref[GROUP] = 0

    def select(slot, b, state):
        src, z, j = state
        valid = src < GROUP
        source = jnp.where(valid, src, 0)
        row = source * SLOT_ROWS + j * ZS + z
        weight = slots_ref[pl.ds(row, 1), :]
        pixel = slots_ref[pl.ds(row + rows, 1), :]
        hot = onehot_rows(pixel, PIX)
        feature = jnp.dot(in_ref[source, SLOT_ROWS:ROWS, :], hot, preferred_element_type=F32)
        val_ref[slot, b] = (feature * weight).astype(BF)
        item = (row + 2 * rows, jnp.where(valid, z, ZS))
        chunks = jnp.right_shift(word_ref[jnp.minimum(src, GROUP)], 3 * z) & 7
        last = j + 1 >= chunks
        j = jnp.where(last, 0, j + 1)
        z = jnp.where(last, z + 1, z)
        wrap = z >= ZS
        z = jnp.where(wrap, 0, z)
        src = jnp.where(wrap, src + 1, src)
        return (src, z, j), item

    def gather(slot, b, item):
        row, place = item
        hot = onehot_rows(slots_ref[pl.ds(row, 1), :], CELLS)
        part = lax.dot_general(
            val_ref[slot, b], hot, (((1,), (1,)), ((), ())), preferred_element_type=F32
        )
        acc_ref[place] = acc_ref[place] + part

    def step(it, carry):
        state, items = carry
        before, now = lax.rem(it, 2), lax.rem(it + 1, 2)
        fresh = []
        for b in range(BATCH_B):
            gather(before, b, items[b])
            state, item = select(now, b, state)
            fresh.append(item)
        return state, tuple(fresh)

    zero = jnp.int32(0)
    batches = (total + BATCH_B - 1) // BATCH_B
    state, items = (zero, zero, zero), []
    for b in range(BATCH_B):
        state, item = select(0, b, state)
        items.append(item)
    _, items = lax.fori_loop(0, batches - 1, step, (state, tuple(items)))
    for b in range(BATCH_B):
        gather(lax.rem(batches - 1, 2), b, items[b])

    left = lax.broadcasted_iota(jnp.int32, (C // 2, 128), 1) < 64
    core = own_core()
    for part, ref in ((core, mine_ref), (1 - core, away_ref)):
        for z in range(ZS // 2):
            for t in range(2):
                a = acc_ref[part * (ZS // 2) + z, : C // 2, t * 128 : (t + 1) * 128]
                b = acc_ref[part * (ZS // 2) + z, C // 2 :, t * 128 : (t + 1) * 128]
                ref[z * 4 + 2 * t] = jnp.where(left, a, pltpu.roll(b, 64, 1)).astype(ref.dtype)
                ref[z * 4 + 2 * t + 1] = jnp.where(left, pltpu.roll(a, 64, 1), b).astype(ref.dtype)


def merge_kernel(in_ref, out_ref):
    parts = []
    for s in range(4):
        total = jnp.zeros((C // 2, 128), F32)
        for z in range(ZS // 2):
            total = total + in_ref[z * 4 + s].astype(F32)
        parts += [total, pltpu.roll(total, 64, 1)]
    stacked = jnp.concatenate(parts, axis=0)
    out_ref[...] = stacked.T[:64, :].astype(BF)


PARAMS = pltpu.CompilerParams(vmem_limit_bytes=12 * 1024 * 1024)
VMEM = pl.BlockSpec(memory_space=pltpu.VMEM)
HBM = pl.BlockSpec(memory_space=pltpu.HBM)
SMEM = pl.BlockSpec(memory_space=pltpu.SMEM)


def send(counts, logits, context, points, cells):
    return pl.pallas_call(
        send_kernel,
        out_shape=pltpu.VMEM((GROUP, ROWS, PIX), BF),
        in_specs=[HBM, HBM, HBM, HBM, HBM],
        out_specs=VMEM,
        scratch_shapes=[
            pltpu.SMEM((STRIPS,), jnp.int32),
            pltpu.VMEM((DEPTH, PIX), F32),
            pltpu.VMEM((C, PIX), BF),
            pltpu.VMEM((STRIPS, CAP), jnp.int32),
            pltpu.VMEM((STRIPS, CAP), jnp.int32),
            pltpu.VMEM((TILES, STRIPS, 128), jnp.int32),
            pltpu.VMEM((TILES, STRIPS, 128), jnp.int32),
            pltpu.VMEM((DEPTH, PIX), BF),
            pltpu.VMEM((TILES, STRIPS, 128), F32),
            pltpu.VMEM((TILES, STRIPS, 128), F32),
            pltpu.VMEM((TILES, STRIPS, 128), F32),
            pltpu.SemaphoreType.DMA((5,)),
        ],
        compiler_params=pltpu.CompilerParams(vmem_limit_bytes=67043328 - 800 * 1024),
        name="send_slots",
    )(counts, logits, context, points, cells)


def pool(slots):
    return pl.pallas_call(
        pool_kernel,
        out_shape=[
            jax.ShapeDtypeStruct((2 * ZS, C // 2, 128), F32),
            jax.ShapeDtypeStruct((2 * ZS, C // 2, 128), BF),
        ],
        in_specs=[VMEM],
        out_specs=[VMEM, VMEM],
        scratch_shapes=[
            pltpu.VMEM((GROUP * SLOT_ROWS, CHUNK), F32),
            pltpu.VMEM((ZS + 1, C, CELLS), F32),
            pltpu.VMEM((2, BATCH_B, C, CHUNK), BF),
            pltpu.SMEM((GROUP + 1,), jnp.int32),
        ],
        compiler_params=PARAMS,
        name="pool_slots",
    )(slots)


def merge(partials):
    return pl.pallas_call(
        merge_kernel,
        out_shape=jax.ShapeDtypeStruct((64, 4 * C), BF),
        in_specs=[VMEM],
        out_specs=VMEM,
        compiler_params=PARAMS,
        name="merge_parts",
    )(partials)


def body(context, depth_logits, send_count, slot_point, slot_cell):
    slots = send(send_count[0, 0], depth_logits[0], context[0], slot_point[0, 0], slot_cell[0, 0])
    slots = lax.all_to_all(slots, ("zl", "x"), 0, 0, tiled=True)
    mine, away = pool(slots)
    theirs = lax.ppermute(away, "core", [(0, 1), (1, 0)])
    partials = (mine + theirs.astype(F32)).astype(BF)
    partials = lax.all_to_all(partials, ("zh", "scene"), 0, 0, tiled=True)
    return merge(partials)


def solution(mesh):
    split = Mesh(mesh.devices.reshape(4, 2, 4, 2, 4), ("zh", "zl", "x", "core", "scene"))
    bev = ("zh", "zl", "x", "core")
    return jax.shard_map(
        body,
        mesh=split,
        in_specs=(
            P("scene", None, bev),
            P("scene", None, bev),
            P("scene", bev, None),
            P("scene", bev, None, None),
            P("scene", bev, None, None),
        ),
        out_specs=P((*bev, "scene"), None),
        check_vma=False,
    )
```

```python
import jax
import jax.numpy as jnp
from jax import lax
from jax.experimental import pallas as pl
from jax.experimental.pallas import tpu as pltpu
from jax.sharding import Mesh, PartitionSpec as P

C = 80
DEPTH = 112
PIX = 256
CELLS = 256
STRIPS = 64
CAP = 1024
CHUNK = 256
NCH = CAP // CHUNK
TILES = CAP // 128
GROUP = 8
ZS = 8
SLOT_ROWS = 3 * ZS * NCH
ROWS = SLOT_ROWS + C
BATCH_A = 50
BATCH_B = 28

BF = jnp.bfloat16
F32 = jnp.float32


def iota16(lanes):
    return lax.broadcasted_iota(jnp.int32, (16, lanes), 0).astype(F32).astype(BF)


def onehot_rows(row, count):
    lanes = row.shape[1]
    base = jnp.broadcast_to(row, (16, lanes)).astype(BF) - iota16(lanes)
    one, zero = jnp.ones((16, lanes), BF), jnp.zeros((16, lanes), BF)
    return jnp.concatenate(
        [jnp.where(base == jnp.asarray(16.0 * g, BF), one, zero) for g in range(count // 16)], axis=0
    ).astype(jnp.float8_e4m3fn)


def send_kernel(
    count_hbm, logits_hbm, ctx_hbm, point_hbm, cell_hbm, out_ref,
    count_ref, logits_ref, ctx_ref, raw_point_ref, raw_cell_ref, point_ref, cell_ref, prob_ref, weight_ref, pixel_ref, target_ref, sems,
):
    pairs = [(count_hbm, count_ref), (logits_hbm, logits_ref), (ctx_hbm, ctx_ref)]
    pairs += [(point_hbm, raw_point_ref), (cell_hbm, raw_cell_ref)]
    copies = [pltpu.make_async_copy(src, dst, sems.at[i]) for i, (src, dst) in enumerate(pairs)]
    for copy in copies:
        copy.start()
    weight_ref[...] = jnp.zeros(weight_ref.shape, F32)
    pixel_ref[...] = jnp.full(pixel_ref.shape, -1.0, F32)
    target_ref[...] = jnp.zeros(target_ref.shape, F32)

    def pieces_of(count):
        return jnp.maximum(jnp.right_shift(count + 127, 7), 1)

    copies[0].wait()
    total = jnp.int32(0)
    for d in range(STRIPS):
        total = total + pieces_of(count_ref[d])

    copies[1].wait()
    logits = logits_ref[...]
    shifted = jnp.exp(logits - jnp.max(logits, axis=0, keepdims=True))
    prob_ref[...] = (shifted / jnp.sum(shifted, axis=0, keepdims=True)).astype(BF)
    sub8 = lax.broadcasted_iota(jnp.int32, (8, 128), 0)
    slot = lax.broadcasted_iota(jnp.int32, (1, 128), 1)
    for copy in copies[2:]:
        copy.wait()
    for t in range(TILES):
        point_ref[t] = raw_point_ref[:, t * 128 : (t + 1) * 128]
        cell_ref[t] = raw_cell_ref[:, t * 128 : (t + 1) * 128]

    def step(_, carry):
        strip, j = carry
        for _ in range(BATCH_A):
            rows, hots = [], []
            for _ in range(2):
                row = jnp.minimum(strip, STRIPS - 1)
                count = count_ref[row]
                point = point_ref[j, pl.ds(row, 1), :]
                rows.append((row, j, count, point))
                hots.append(onehot_rows((point & (PIX - 1)).astype(F32), PIX))
                last = j + 1 >= pieces_of(count)
                strip = jnp.where(last, strip + 1, strip)
                j = jnp.where(last, 0, j + 1)
            hot = jnp.concatenate(hots, axis=1)
            columns = jnp.dot(prob_ref[...], hot, preferred_element_type=F32)
            for half, (row, piece, count, point) in enumerate(rows):
                bin_id = jnp.broadcast_to(jnp.right_shift(point, 8), (8, 128))
                column = columns[:, half * 128 : (half + 1) * 128]
                level = [column[8 * g : 8 * g + 8, :] for g in range(DEPTH // 8)]
                for bit in (8, 16, 32, 64):
                    upper = (bin_id & bit) != 0
                    level = [
                        jnp.where(upper, level[i + 1], level[i]) if i + 1 < len(level) else level[i]
                        for i in range(0, len(level), 2)
                    ]
                weight = jnp.sum(jnp.where((bin_id & 7) == sub8, level[0], 0.0), axis=0, keepdims=True)
                pixel = jnp.where(slot + piece * 128 < count, point & (PIX - 1), -1).astype(F32)
                cell = cell_ref[piece, pl.ds(row, 1), :].astype(F32)
                inside = jnp.right_shift(row, 1)
                place = (inside & (GROUP - 1)) * ZS + (row & 1) * (ZS // 2) + jnp.right_shift(row, 4)
                for ref, value in ((weight_ref, weight), (pixel_ref, pixel), (target_ref, cell)):
                    ref[piece, pl.ds(place, 1), :] = value
        return strip, j

    steps = (total + 2 * BATCH_A - 1) // (2 * BATCH_A)
    lax.fori_loop(0, steps, step, (jnp.int32(0), jnp.int32(0)))

    context = ctx_ref[...]
    for dest in range(GROUP):
        for kind, ref in enumerate((weight_ref, pixel_ref, target_ref)):
            for half in range(2):
                stacked = jnp.concatenate(
                    [ref[2 * i + half, dest * ZS : (dest + 1) * ZS, :] for i in range(NCH)], axis=0
                )
                out_ref[
                    dest, kind * ZS * NCH : (kind + 1) * ZS * NCH, half * 128 : (half + 1) * 128
                ] = stacked.astype(BF)
        out_ref[dest, SLOT_ROWS:ROWS, :] = context


def own_core():
    return lax.axis_index("core")


def pool_kernel(in_ref, mine_ref, away_ref, slots_ref, acc_ref, val_ref, word_ref):
    for src in range(GROUP):
        slots_ref[src * SLOT_ROWS : (src + 1) * SLOT_ROWS, :] = in_ref[src, :SLOT_ROWS, :].astype(F32)
    acc_ref[...] = jnp.zeros(acc_ref.shape, F32)

    rows = ZS * NCH
    lane0 = lax.broadcasted_iota(jnp.int32, (ZS, 128), 1) == 0
    digit = jnp.left_shift(1, 3 * lax.broadcasted_iota(jnp.int32, (ZS, 128), 0)).astype(F32)
    everywhere = jnp.zeros((ZS, 128), F32)
    for src in range(GROUP):
        live = jnp.zeros((ZS, 128), F32)
        for j in range(NCH):
            first = slots_ref[src * SLOT_ROWS + rows + j * ZS : src * SLOT_ROWS + rows + (j + 1) * ZS, :128]
            on = first >= 0.0
            if j == 0:
                on = on | True
            live = live + jnp.where(lane0 & on, 1.0, 0.0)
        word_ref[src] = jnp.sum(live * digit).astype(jnp.int32)
        everywhere = everywhere + live
    total = jnp.sum(everywhere).astype(jnp.int32)
    word_ref[GROUP] = 0

    def select(slot, b, state):
        src, z, j = state
        valid = src < GROUP
        source = jnp.where(valid, src, 0)
        row = source * SLOT_ROWS + j * ZS + z
        weight = slots_ref[pl.ds(row, 1), :]
        pixel = slots_ref[pl.ds(row + rows, 1), :]
        hot = onehot_rows(pixel, PIX)
        feature = jnp.dot(in_ref[source, SLOT_ROWS:ROWS, :], hot, preferred_element_type=F32)
        val_ref[slot, b] = (feature * weight).astype(BF)
        item = (row + 2 * rows, jnp.where(valid, z, ZS))
        chunks = jnp.right_shift(word_ref[jnp.minimum(src, GROUP)], 3 * z) & 7
        last = j + 1 >= chunks
        j = jnp.where(last, 0, j + 1)
        z = jnp.where(last, z + 1, z)
        wrap = z >= ZS
        z = jnp.where(wrap, 0, z)
        src = jnp.where(wrap, src + 1, src)
        return (src, z, j), item

    def gather(slot, b, item):
        row, place = item
        hot = onehot_rows(slots_ref[pl.ds(row, 1), :], CELLS)
        part = lax.dot_general(
            val_ref[slot, b], hot, (((1,), (1,)), ((), ())), preferred_element_type=F32
        )
        acc_ref[place] = acc_ref[place] + part

    def step(it, carry):
        state, items = carry
        before, now = lax.rem(it, 2), lax.rem(it + 1, 2)
        fresh = []
        for b in range(BATCH_B):
            gather(before, b, items[b])
            state, item = select(now, b, state)
            fresh.append(item)
        return state, tuple(fresh)

    zero = jnp.int32(0)
    batches = (total + BATCH_B - 1) // BATCH_B
    state, items = (zero, zero, zero), []
    for b in range(BATCH_B):
        state, item = select(0, b, state)
        items.append(item)
    _, items = lax.fori_loop(0, batches - 1, step, (state, tuple(items)))
    for b in range(BATCH_B):
        gather(lax.rem(batches - 1, 2), b, items[b])

    left = lax.broadcasted_iota(jnp.int32, (C // 2, 128), 1) < 64
    core = own_core()
    for part, ref in ((core, mine_ref), (1 - core, away_ref)):
        for z in range(ZS // 2):
            for t in range(2):
                a = acc_ref[part * (ZS // 2) + z, : C // 2, t * 128 : (t + 1) * 128]
                b = acc_ref[part * (ZS // 2) + z, C // 2 :, t * 128 : (t + 1) * 128]
                ref[z * 4 + 2 * t] = jnp.where(left, a, pltpu.roll(b, 64, 1)).astype(ref.dtype)
                ref[z * 4 + 2 * t + 1] = jnp.where(left, pltpu.roll(a, 64, 1), b).astype(ref.dtype)


def merge_kernel(in_ref, out_ref):
    parts = []
    for s in range(4):
        total = jnp.zeros((C // 2, 128), F32)
        for z in range(ZS // 2):
            total = total + in_ref[z * 4 + s].astype(F32)
        parts += [total, pltpu.roll(total, 64, 1)]
    stacked = jnp.concatenate(parts, axis=0)
    out_ref[...] = stacked.T[:64, :].astype(BF)


PARAMS = pltpu.CompilerParams(vmem_limit_bytes=12 * 1024 * 1024)
VMEM = pl.BlockSpec(memory_space=pltpu.VMEM)
HBM = pl.BlockSpec(memory_space=pltpu.HBM)
SMEM = pl.BlockSpec(memory_space=pltpu.SMEM)


def send(counts, logits, context, points, cells):
    return pl.pallas_call(
        send_kernel,
        out_shape=pltpu.VMEM((GROUP, ROWS, PIX), BF),
        in_specs=[HBM, HBM, HBM, HBM, HBM],
        out_specs=VMEM,
        scratch_shapes=[
            pltpu.SMEM((STRIPS,), jnp.int32),
            pltpu.VMEM((DEPTH, PIX), F32),
            pltpu.VMEM((C, PIX), BF),
            pltpu.VMEM((STRIPS, CAP), jnp.int32),
            pltpu.VMEM((STRIPS, CAP), jnp.int32),
            pltpu.VMEM((TILES, STRIPS, 128), jnp.int32),
            pltpu.VMEM((TILES, STRIPS, 128), jnp.int32),
            pltpu.VMEM((DEPTH, PIX), BF),
            pltpu.VMEM((TILES, STRIPS, 128), F32),
            pltpu.VMEM((TILES, STRIPS, 128), F32),
            pltpu.VMEM((TILES, STRIPS, 128), F32),
            pltpu.SemaphoreType.DMA((5,)),
        ],
        compiler_params=pltpu.CompilerParams(vmem_limit_bytes=67043328 - 800 * 1024),
        name="send_slots",
    )(counts, logits, context, points, cells)


def pool(slots):
    return pl.pallas_call(
        pool_kernel,
        out_shape=[
            jax.ShapeDtypeStruct((2 * ZS, C // 2, 128), F32),
            jax.ShapeDtypeStruct((2 * ZS, C // 2, 128), BF),
        ],
        in_specs=[VMEM],
        out_specs=[VMEM, VMEM],
        scratch_shapes=[
            pltpu.VMEM((GROUP * SLOT_ROWS, CHUNK), F32),
            pltpu.VMEM((ZS + 1, C, CELLS), F32),
            pltpu.VMEM((2, BATCH_B, C, CHUNK), BF),
            pltpu.SMEM((GROUP + 1,), jnp.int32),
        ],
        compiler_params=PARAMS,
        name="pool_slots",
    )(slots)


def merge(partials):
    return pl.pallas_call(
        merge_kernel,
        out_shape=jax.ShapeDtypeStruct((64, 4 * C), BF),
        in_specs=[VMEM],
        out_specs=VMEM,
        compiler_params=PARAMS,
        name="merge_parts",
    )(partials)


def body(context, depth_logits, send_count, slot_point, slot_cell):
    slots = send(send_count[0, 0], depth_logits[0], context[0], slot_point[0, 0], slot_cell[0, 0])
    slots = lax.all_to_all(slots, ("zl", "x"), 0, 0, tiled=True)
    mine, away = pool(slots)
    theirs = lax.ppermute(away, "core", [(0, 1), (1, 0)])
    partials = (mine + theirs.astype(F32)).astype(BF)
    partials = lax.all_to_all(partials, ("zh", "scene"), 0, 0, tiled=True)
    return merge(partials)


def solution(mesh):
    split = Mesh(mesh.devices.reshape(4, 2, 4, 2, 4), ("zh", "zl", "x", "core", "scene"))
    bev = ("zh", "zl", "x", "core")
    return jax.shard_map(
        body,
        mesh=split,
        in_specs=(
            P("scene", None, bev),
            P("scene", None, bev),
            P("scene", bev, None),
            P("scene", bev, None, None),
            P("scene", bev, None, None),
        ),
        out_specs=P((*bev, "scene"), None),
        check_vma=False,
    )
```
